32 devices in a mesh: sub: 16 (over z, y, core), tm: 2 (over x).
Axes of the slice: x: 2, y: 2, z: 4, core: 2. Of those that a mesh axis runs over, the one named last changes fastest.
Arguments:
- voltages: bfloat16 [192, 2, 96, 2048], P('sub', None, None, 'tm'), may hold values from -6 to 6
- pointing_table: bfloat16 [192, 2, 320, 96], P('sub'), may hold values from -0.4375 to 0.4375
- beam_pointing: int32 [256], replicated, may hold values from 0 to 319
- subband_order: int32 [192], replicated, may hold values from 0 to 191, each once
- live_subbands: int32 [1], replicated, may hold values from 152 to 192
- filter_taps: float32 [16, 16], replicated, may hold values from -0.36 to 0.36
Outputs:
- synthesised: bfloat16 [256, 12, 2, 32768], P('sub', None, None, 'tm')
The draws below stay inside these ranges and needn't reach their ends.
Inputs may be any that keep to these rules, and one draw needn't show every extreme that they name: `subband_order`: each slot is named by exactly one frequency.
All inputs are finite; a program needn't handle non-finite values.
Results may differ from the reference program's by a relative error of at most 0.0052.
Values may be sent and summed in bfloat16 or wider, within the bound.
A program may use at most 192 MiB of HBM per device.

```python
import math
import jax
import jax.numpy as jnp
from jax import lax

INPUTS = 96
BEAMS = 256
POINTINGS = 320
CHAN = 16
TAPS = 16
SUBBANDS = 192
TIME = 2048


def draw_live_subbands(key, part):
    span = 2 * CHAN + CHAN // 2
    raw = jax.random.randint(jax.random.fold_in(key, 7919), (1,), -span, span + 1, dtype=jnp.int32)
    missing = jnp.maximum(raw, 0)
    return (SUBBANDS - missing).astype(jnp.int32)


def place_ends(drawn, rng, smallest, top_value):
    longest = drawn.shape.index(max(drawn.shape))
    spots = []
    for shift in (0, 1):
        where = [jax.random.randint(jax.random.fold_in(rng, axis), (), 0, length) for axis, length in enumerate(drawn.shape)]
        where[longest] = (where[longest] + shift) % drawn.shape[longest]
        spots.append(tuple(where))
    return drawn.at[spots[0]].set(smallest).at[spots[1]].set(top_value)


def levels(key, shape, cuts, least, top_value):
    def one(axis_at, blocks):
        steps = jax.random.uniform(jax.random.fold_in(jax.random.fold_in(key, 6), axis_at), (blocks,), jnp.float32, least / len(cuts), top_value / len(cuts))
        return jnp.repeat(jnp.exp(steps), shape[axis_at] // blocks).reshape((-1,) + (1,) * (len(shape) - axis_at - 1))

    loudness = one(*cuts[0])
    for cut in cuts[1:]:
        loudness = loudness * one(*cut)
    return loudness


def gaussian(own_key, dims, spread, bound, pieces=(), held_as=jnp.bfloat16):
    array = spread * jax.random.normal(own_key, dims, jnp.float32)
    if pieces:
        array = array * levels(own_key, dims, pieces, -0.22, 0.18)
    return jnp.clip(array, -bound, bound).astype(held_as)


def setup_inputs(seed: int = 0) -> dict:
    key_of = jax.random.split(jax.random.key(seed), 7)
    return {
        "voltages": gaussian(key_of[0], (SUBBANDS, 2, INPUTS, TIME), 1.0, 6.0, ((0, 16), (3, 2))),
        "pointing_table": gaussian(key_of[1], (SUBBANDS, 2, POINTINGS, INPUTS), (2 * INPUTS) ** -0.5, 0.4375, ((0, 16),)),
        "beam_pointing": place_ends(jax.random.randint(key_of[2], (BEAMS,), 0, POINTINGS), jax.random.fold_in(key_of[2], 1), 0, POINTINGS - 1).astype(jnp.int32),
        "subband_order": jax.random.permutation(key_of[3], SUBBANDS).astype(jnp.int32),
        "live_subbands": draw_live_subbands(jax.random.fold_in(key_of[6], 71), 0),
        "filter_taps": gaussian(key_of[5], (TAPS, CHAN), 0.06, 0.36, (), jnp.float32),
    }


def inverse_table(channel_count):
    channel_index = jnp.arange(channel_count, dtype=jnp.int32)
    phase = (jnp.outer(channel_index, channel_index) % channel_count).astype(jnp.float32) * (2.0 * math.pi / channel_count)
    cosine = jnp.cos(phase).astype(jnp.bfloat16)
    sine_table = jnp.sin(phase).astype(jnp.bfloat16)
    upper_rows = jnp.stack([cosine, -sine_table], axis=1)
    lower_rows = jnp.stack([sine_table, cosine], axis=1)
    return jnp.stack([upper_rows, lower_rows], axis=0)


def reference(voltages, pointing_table, beam_pointing, subband_order, live_subbands, filter_taps):
    highest = lax.Precision.HIGHEST

    def form_subband(subband_pair):
        table_rows, signal = subband_pair
        chosen = jnp.take(table_rows, beam_pointing, axis=1).astype(jnp.float32)
        signal = signal.astype(jnp.float32)
        real_part = jnp.dot(chosen[0], signal[0], precision=highest) - jnp.dot(chosen[1], signal[1], precision=highest)
        imag_part = jnp.dot(chosen[1], signal[0], precision=highest) + jnp.dot(chosen[0], signal[1], precision=highest)
        return jnp.stack([real_part, imag_part], axis=1).astype(jnp.bfloat16)

    formed = lax.map(form_subband, (pointing_table, voltages))
    inverse_rows = inverse_table(CHAN).astype(jnp.float32)
    live_mask = jnp.arange(SUBBANDS, dtype=jnp.int32) < live_subbands[0]
    length = formed.shape[3]

    def synth_beam(beam_index):
        beam_rows = lax.dynamic_index_in_dim(formed, beam_index, 1, keepdims=False)
        spectrum = jnp.take(beam_rows, subband_order, axis=0)
        spectrum = jnp.where(live_mask[:, None, None], spectrum, jnp.zeros_like(spectrum))
        grouped = spectrum.astype(jnp.float32).reshape(SUBBANDS // CHAN, CHAN, 2, length)
        channels = jnp.einsum('qkpc,gcpt->gqkt', inverse_rows, grouped, precision=highest)
        extended = jnp.pad(channels, ((0, 0), (0, 0), (0, 0), (TAPS - 1, 0)))
        running = jnp.zeros_like(channels)
        for tap_index in range(TAPS):
            offset = TAPS - 1 - tap_index
            running = running + filter_taps[tap_index][:, None] * extended[..., offset:offset + length]
        return jnp.swapaxes(running, 2, 3).reshape(SUBBANDS // CHAN, 2, length * CHAN).astype(jnp.bfloat16)

    return lax.map(synth_beam, jnp.arange(BEAMS, dtype=jnp.int32))
```

```python
import functools
import math

import jax
import jax.numpy as jnp
from jax import lax
from jax.experimental import pallas as pl
from jax.experimental.pallas import tpu as pltpu
from jax.sharding import PartitionSpec as P

LANES = 128
VMEM = 60 * 1024 * 1024


def inverse_table(channel_count):
    channel_index = jnp.arange(channel_count, dtype=jnp.int32)
    phase = (jnp.outer(channel_index, channel_index) % channel_count).astype(jnp.float32) * (
        2.0 * math.pi / channel_count
    )
    cosine = jnp.cos(phase).astype(jnp.bfloat16)
    sine_table = jnp.sin(phase).astype(jnp.bfloat16)
    upper_rows = jnp.stack([cosine, -sine_table], axis=1)
    lower_rows = jnp.stack([sine_table, cosine], axis=1)
    return jnp.stack([upper_rows, lower_rows], axis=0)


def synthesis_matrix(filter_taps, inner, reach):
    tap_count, chan = filter_taps.shape
    table = inverse_table(chan).astype(jnp.float32)
    delta = jnp.arange(reach)[:, None, None]
    tl_in = jnp.arange(inner)[None, :, None]
    tl_out = jnp.arange(inner)[None, None, :]
    tap = inner * delta + tl_out - tl_in
    inside = (tap >= 0) & (tap < tap_count)
    taps = jnp.where(inside[..., None], filter_taps[jnp.clip(tap, 0, tap_count - 1)], 0.0)
    full = (
        taps[:, None, :, None, None, :, :]
        * table.transpose(2, 3, 0, 1)[None, :, None, :, :, None, :]
    )
    return full.reshape(reach * 2 * inner * chan, 2 * inner * chan).astype(jnp.bfloat16)


def form_kernel(inner, group, hot_ref, perm_ref, table_ref, volt_ref, rim_ref, *outs):
    chunks = outs[:-1]
    rim_out = outs[-1]
    f32, bf16 = jnp.float32, jnp.bfloat16
    real, imag = table_ref[0, 0], table_ref[0, 1]
    both = jnp.concatenate(
        [
            jnp.concatenate([real, -imag], axis=1),
            jnp.concatenate([imag, real], axis=1),
        ],
        axis=0,
    )
    weights = jnp.dot(hot_ref[...], both, preferred_element_type=f32).astype(bf16)
    rim_out[0] = jnp.dot(weights, rim_ref[0], preferred_element_type=f32).astype(bf16)
    signal = jnp.dot(volt_ref[0], perm_ref[...], preferred_element_type=f32).astype(bf16)
    rows = weights.shape[0] // len(chunks)
    for h, out in enumerate(chunks):
        formed = jnp.dot(
            weights[h * rows : (h + 1) * rows], signal, preferred_element_type=f32
        ).astype(bf16)
        for d in range(out.shape[0]):
            for tl in range(inner):
                out[d, 0, tl] = formed[
                    2 * d * group : 2 * (d + 1) * group, tl * LANES : (tl + 1) * LANES
                ]


def synth_kernel(inner, chan, group, reach, order_ref, live_ref, z_ref, rim_ref, mat_ref, *rest):
    out_ref, held, wide, line, stacked, made, sems = rest[-7:]
    g = pl.program_id(0)
    count = pl.num_programs(0)
    f32, bf16 = jnp.float32, jnp.bfloat16

    def fetch(step, slot):
        return [
            pltpu.make_async_copy(
                z_ref.at[order_ref[step * chan + c]], held.at[slot, c], sems.at[slot]
            )
            for c in range(chan)
        ]

    slot = lax.rem(g, 2)

    @pl.when(g == 0)
    def _():
        for copy in fetch(0, 0):
            copy.start()

    @pl.when(g + 1 < count)
    def _():
        for copy in fetch(g + 1, 1 - slot):
            copy.start()

    for copy in fetch(g, slot):
        copy.wait()

    pair = 2 * group
    for c in range(chan):
        alive = g * chan + c < live_ref[0]
        for tl in range(inner):
            block = held[slot, c, tl].astype(f32)
            wide[tl, c * pair : (c + 1) * pair, :] = jnp.where(alive, block, 0.0)

    width = inner * chan

    def turn(b, carry):
        base = pl.multiple_of(b * LANES, LANES)
        for p in range(2):
            rows = [
                wide[tl, pl.ds(p * group + b, chan, stride=pair), :] for tl in range(inner)
            ]
            line[p, 8 : 8 + LANES, :] = jnp.concatenate(rows, axis=0).T
            line[p, 8 - (reach - 1) : 8, :] = rim_ref[0, b, p]
            for delta in range(reach):
                at = (2 * delta + p) * width
                stacked[pl.ds(base, LANES), at : at + width] = line[
                    p, 8 - delta : 8 - delta + LANES, :
                ].astype(bf16)
        return carry

    lax.fori_loop(0, group, turn, 0, unroll=2)

    def emit(b, carry):
        base = pl.multiple_of(b * 2 * LANES, 2 * LANES)
        out = jnp.dot(
            stacked[pl.ds(base, 2 * LANES), :], mat_ref[...], preferred_element_type=f32
        )
        for i in range(2):
            for q in range(2):
                made[i, q * LANES : (q + 1) * LANES, :] = out[
                    i * LANES : (i + 1) * LANES, q * width : (q + 1) * width
                ]
        for i in range(2):
            for tb in range(LANES):
                both = made[i, pl.ds(tb, 2, stride=LANES), :].astype(bf16)
                out_ref[2 * b + i, 0, :, tb * LANES : (tb + 1) * LANES] = both
        return carry

    lax.fori_loop(0, group // 2, emit, 0)


def on_device(voltages, pointing_table, beam_pointing, subband_order, live_subbands, filter_taps):
    local_subbands, _, inputs, local_time = voltages.shape
    pointings = pointing_table.shape[2]
    beam_count = beam_pointing.shape[0]
    slots = subband_order.shape[0]
    tap_count, chan = filter_taps.shape
    inner = LANES // chan
    assert local_time == inner * LANES
    reach = 1 + -(-(tap_count - 1) // inner)
    rim_len = (reach - 1) * inner
    devices = lax.axis_size("sub")
    beam_part = beam_count // devices
    group = min(8, beam_part)
    chunk_count = beam_part // group
    bands = slots // chan

    signal = voltages.reshape(local_subbands, 2 * inputs, local_time)
    times = range(lax.axis_size("tm"))
    route = [(i - 1, i) for i in times if i > 0]
    rim = lax.ppermute(signal[:, :, local_time - rim_len :], "tm", route)
    rim = jnp.pad(rim, ((0, 0), (0, 0), (0, LANES - rim_len)))

    picks = beam_pointing.reshape(devices, chunk_count, 1, group).swapaxes(0, 1)
    wanted = (picks + pointings * jnp.arange(2)[:, None]).reshape(-1)
    hot = (wanted[:, None] == jnp.arange(2 * pointings)[None, :]).astype(jnp.bfloat16)
    source = jnp.arange(local_time, dtype=jnp.int32)
    place = (source % inner) * LANES + source // inner
    perm = (place[:, None] == source[None, :]).astype(jnp.bfloat16)

    piece = (devices, local_subbands, inner, 2 * group, LANES)
    made = pl.pallas_call(
        functools.partial(form_kernel, inner, group),
        grid=(local_subbands,),
        in_specs=[
            pl.BlockSpec(hot.shape, lambda s: (0, 0)),
            pl.BlockSpec(perm.shape, lambda s: (0, 0)),
            pl.BlockSpec((1, 2, pointings, inputs), lambda s: (s, 0, 0, 0)),
            pl.BlockSpec((1, 2 * inputs, local_time), lambda s: (s, 0, 0)),
            pl.BlockSpec((1, 2 * inputs, LANES), lambda s: (s, 0, 0)),
        ],
        out_specs=[
            pl.BlockSpec((devices, 1, inner, 2 * group, LANES), lambda s: (0, s, 0, 0, 0))
        ]
        * chunk_count
        + [pl.BlockSpec((1, 2 * beam_count, LANES), lambda s: (s, 0, 0))],
        out_shape=[jax.ShapeDtypeStruct(piece, jnp.bfloat16)] * chunk_count
        + [jax.ShapeDtypeStruct((local_subbands, 2 * beam_count, LANES), jnp.bfloat16)],
        compiler_params=pltpu.CompilerParams(vmem_limit_bytes=VMEM),
        cost_estimate=pl.CostEstimate(
            flops=12_000_000_000, bytes_accessed=20_000_000, transcendentals=0
        ),
        name="form",
    )(hot, perm, pointing_table, signal, rim)

    mat = synthesis_matrix(filter_taps, inner, reach)

    edge = made[-1][:, :, :rim_len].reshape(
        local_subbands, chunk_count, devices, 2 * group * rim_len
    )
    edge = edge.transpose(2, 0, 1, 3).reshape(devices, local_subbands, -1)
    edge = lax.all_to_all(edge, "sub", split_axis=0, concat_axis=0, tiled=True)
    edge = jnp.take(edge.reshape(slots, -1), subband_order, axis=0)
    live_mask = jnp.arange(slots, dtype=jnp.int32) < live_subbands[0]
    edge = jnp.where(live_mask[:, None], edge.astype(jnp.float32), 0.0)
    edge = edge.reshape(bands, chan, chunk_count, 2, group, reach - 1, inner)
    edge = edge.transpose(2, 0, 4, 3, 5, 6, 1).reshape(
        chunk_count, bands, group, 2, reach - 1, inner * chan
    )

    result = None
    for h in range(chunk_count):
        z = lax.all_to_all(made[h], "sub", split_axis=0, concat_axis=0, tiled=True)
        z = z.reshape(slots, inner, 2 * group, LANES)
        operands = [subband_order, live_subbands, z, edge[h], mat]
        in_specs = [
            pl.BlockSpec(memory_space=pl.ANY),
            pl.BlockSpec((1, group, 2, reach - 1, LANES), lambda g, *_: (g, 0, 0, 0, 0)),
            pl.BlockSpec(mat.shape, lambda g, *_: (0, 0)),
        ]
        alias = {}
        if result is not None:
            operands.append(result)
            in_specs.append(pl.BlockSpec(memory_space=pl.ANY))
            alias = {5: 0}
        result = pl.pallas_call(
            functools.partial(synth_kernel, inner, chan, group, reach),
            grid_spec=pltpu.PrefetchScalarGridSpec(
                num_scalar_prefetch=2,
                grid=(bands,),
                in_specs=in_specs,
                out_specs=pl.BlockSpec(
                    (group, 1, 2, local_time * chan), functools.partial(lambda h, g, *_: (h, g, 0, 0), h)
                ),
                scratch_shapes=[
                    pltpu.VMEM((2, chan, inner, 2 * group, LANES), jnp.bfloat16),
                    pltpu.VMEM((inner, chan * 2 * group, LANES), jnp.float32),
                    pltpu.VMEM((2, 8 + LANES, LANES), jnp.float32),
                    pltpu.VMEM((group * LANES, mat.shape[0]), jnp.bfloat16),
                    pltpu.VMEM((2, 2 * LANES, LANES), jnp.float32),
                    pltpu.SemaphoreType.DMA((2,)),
                ],
            ),
            out_shape=jax.ShapeDtypeStruct((beam_part, bands, 2, local_time * chan), jnp.bfloat16),
            input_output_aliases=alias,
            compiler_params=pltpu.CompilerParams(vmem_limit_bytes=VMEM),
            cost_estimate=pl.CostEstimate(
                flops=10_000_000_000, bytes_accessed=13_000_000, transcendentals=0
            ),
            name="synth",
        )(*operands)

    return result


def solution(mesh):
    in_specs = (P("sub", None, None, "tm"), P("sub", None, None, None), P(), P(), P(), P())
    out_specs = P("sub", None, None, "tm")
    return jax.shard_map(
        on_device, mesh=mesh, in_specs=in_specs, out_specs=out_specs, check_vma=False
    )
```

```python
import functools
import math

import jax
import jax.numpy as jnp
from jax import lax
from jax.experimental import pallas as pl
from jax.experimental.pallas import tpu as pltpu
from jax.sharding import PartitionSpec as P

LANES = 128
VMEM = 60 * 1024 * 1024


def inverse_table(channel_count):
    channel_index = jnp.arange(channel_count, dtype=jnp.int32)
    phase = (jnp.outer(channel_index, channel_index) % channel_count).astype(jnp.float32) * (
        2.0 * math.pi / channel_count
    )
    cosine = jnp.cos(phase).astype(jnp.bfloat16)
    sine_table = jnp.sin(phase).astype(jnp.bfloat16)
    upper_rows = jnp.stack([cosine, -sine_table], axis=1)
    lower_rows = jnp.stack([sine_table, cosine], axis=1)
    return jnp.stack([upper_rows, lower_rows], axis=0)


def synthesis_matrix(filter_taps, inner, reach):
    tap_count, chan = filter_taps.shape
    table = inverse_table(chan).astype(jnp.float32)
    delta = jnp.arange(reach)[:, None, None]
    tl_in = jnp.arange(inner)[None, :, None]
    tl_out = jnp.arange(inner)[None, None, :]
    tap = inner * delta + tl_out - tl_in
    inside = (tap >= 0) & (tap < tap_count)
    taps = jnp.where(inside[..., None], filter_taps[jnp.clip(tap, 0, tap_count - 1)], 0.0)
    full = (
        taps[:, None, :, None, None, :, :]
        * table.transpose(2, 3, 0, 1)[None, :, None, :, :, None, :]
    )
    return full.reshape(reach * 2 * inner * chan, 2 * inner * chan).astype(jnp.bfloat16)


def form_kernel(inner, groups, with_rim, hot_ref, perm_ref, table_ref, volt_ref, *rest):
    chunks = rest[-len(groups) :]
    f32, bf16 = jnp.float32, jnp.bfloat16
    real, imag = table_ref[0, 0], table_ref[0, 1]
    both = jnp.concatenate(
        [
            jnp.concatenate([real, -imag], axis=1),
            jnp.concatenate([imag, real], axis=1),
        ],
        axis=0,
    )
    weights = jnp.dot(hot_ref[...], both, preferred_element_type=f32).astype(bf16)
    if with_rim:
        rim_ref, rim_out = rest[0], rest[1]
        rim_out[0] = jnp.dot(weights, rim_ref[0], preferred_element_type=f32).astype(bf16)
    signal = jnp.dot(volt_ref[0], perm_ref[...], preferred_element_type=f32).astype(bf16)
    start = 0 if with_rim else hot_ref.shape[0] - 2 * sum(groups) * chunks[0].shape[0]
    for group, out in zip(groups, chunks):
        rows = 2 * group * out.shape[0]
        formed = jnp.dot(
            weights[start : start + rows], signal, preferred_element_type=f32
        ).astype(bf16)
        start += rows
        for d in range(out.shape[0]):
            for tl in range(inner):
                out[d, 0, tl] = formed[
                    2 * d * group : 2 * (d + 1) * group, tl * LANES : (tl + 1) * LANES
                ]


def synth_kernel(
    inner, chan, group, reach, local, order_ref, live_ref, z_ref, rim_ref, mat_ref, *rest
):
    out_ref, held, wide, line, stacked, made, sems = rest[-7:]
    g = pl.program_id(0)
    count = pl.num_programs(0)
    f32, bf16 = jnp.float32, jnp.bfloat16

    def fetch(step, slot):
        named = [order_ref[step * chan + c] for c in range(chan)]
        return [
            pltpu.make_async_copy(
                z_ref.at[lax.div(at, local), pl.ds(lax.rem(at, local) * inner, inner)],
                held.at[slot, c],
                sems.at[slot],
            )
            for c, at in enumerate(named)
        ]

    slot = lax.rem(g, 2)

    @pl.when(g == 0)
    def _():
        for copy in fetch(0, 0):
            copy.start()

    @pl.when(g + 1 < count)
    def _():
        for copy in fetch(g + 1, 1 - slot):
            copy.start()

    for copy in fetch(g, slot):
        copy.wait()

    pair = 2 * group
    for c in range(chan):
        alive = g * chan + c < live_ref[0]
        for tl in range(inner):
            block = held[slot, c, tl].astype(f32)
            wide[tl, c * pair : (c + 1) * pair, :] = jnp.where(alive, block, 0.0)

    width = inner * chan

    def turn(b, carry):
        base = pl.multiple_of(b * LANES, LANES)
        for p in range(2):
            rows = [
                wide[tl, pl.ds(p * group + b, chan, stride=pair), :] for tl in range(inner)
            ]
            line[p, 8 : 8 + LANES, :] = jnp.concatenate(rows, axis=0).T
            line[p, 8 - (reach - 1) : 8, :] = rim_ref[0, b, p]
            for delta in range(reach):
                at = (2 * delta + p) * width
                stacked[pl.ds(base, LANES), at : at + width] = line[
                    p, 8 - delta : 8 - delta + LANES, :
                ].astype(bf16)
        return carry

    lax.fori_loop(0, group, turn, 0, unroll=2)

    def emit(b, carry):
        base = pl.multiple_of(b * 2 * LANES, 2 * LANES)
        out = jnp.dot(
            stacked[pl.ds(base, 2 * LANES), :], mat_ref[...], preferred_element_type=f32
        )
        for i in range(2):
            for q in range(2):
                made[i, q * LANES : (q + 1) * LANES, :] = out[
                    i * LANES : (i + 1) * LANES, q * width : (q + 1) * width
                ]
        for i in range(2):
            for tb in range(LANES):
                both = made[i, pl.ds(tb, 2, stride=LANES), :].astype(bf16)
                out_ref[2 * b + i, 0, :, tb * LANES : (tb + 1) * LANES] = both
        return carry

    lax.fori_loop(0, group // 2, emit, 0)


def on_device(voltages, pointing_table, beam_pointing, subband_order, live_subbands, filter_taps):
    local_subbands, _, inputs, local_time = voltages.shape
    pointings = pointing_table.shape[2]
    beam_count = beam_pointing.shape[0]
    slots = subband_order.shape[0]
    tap_count, chan = filter_taps.shape
    inner = LANES // chan
    assert local_time == inner * LANES
    reach = 1 + -(-(tap_count - 1) // inner)
    rim_len = (reach - 1) * inner
    devices = lax.axis_size("sub")
    beam_part = beam_count // devices
    quarter = beam_part // 4
    if beam_part % 8 == 0:
        groups, firsts = [quarter, 2 * quarter, quarter], [0, 2 * quarter, quarter]
    else:
        groups, firsts = [beam_part], [0]
    starts = [sum(groups[:h]) for h in range(len(groups))]
    bands = slots // chan

    signal = voltages.reshape(local_subbands, 2 * inputs, local_time)
    times = range(lax.axis_size("tm"))
    route = [(i - 1, i) for i in times if i > 0]
    rim = lax.ppermute(signal[:, :, local_time - rim_len :], "tm", route)
    rim = jnp.pad(rim, ((0, 0), (0, 0), (0, LANES - rim_len)))

    picks = beam_pointing.reshape(devices, beam_part)
    wanted = jnp.concatenate(
        [
            (
                picks[:, None, first : first + group]
                + pointings * jnp.arange(2, dtype=jnp.int32)[:, None]
            ).reshape(-1)
            for first, group in zip(firsts, groups)
        ]
    )
    hot = (wanted[:, None] == jnp.arange(2 * pointings)[None, :]).astype(jnp.bfloat16)
    source = jnp.arange(local_time, dtype=jnp.int32)
    place = (source % inner) * LANES + source // inner
    perm = (place[:, None] == source[None, :]).astype(jnp.bfloat16)

    def form(groups, signal, rim):
        with_rim = rim is not None
        pieces = [(devices, local_subbands, inner, 2 * group, LANES) for group in groups]
        rim_size = (local_subbands, hot.shape[0], LANES)
        return pl.pallas_call(
            functools.partial(form_kernel, inner, groups, with_rim),
            grid=(local_subbands,),
            in_specs=[
                pl.BlockSpec(hot.shape, lambda s: (0, 0)),
                pl.BlockSpec(perm.shape, lambda s: (0, 0)),
                pl.BlockSpec((1, 2, pointings, inputs), lambda s: (s, 0, 0, 0)),
                pl.BlockSpec((1, 2 * inputs, local_time), lambda s: (s, 0, 0)),
            ]
            + [pl.BlockSpec((1, 2 * inputs, LANES), lambda s: (s, 0, 0))] * with_rim,
            out_specs=[pl.BlockSpec((1,) + rim_size[1:], lambda s: (s, 0, 0))] * with_rim
            + [
                pl.BlockSpec((size[0], 1) + size[2:], lambda s: (0, s, 0, 0, 0))
                for size in pieces
            ],
            out_shape=[jax.ShapeDtypeStruct(rim_size, jnp.bfloat16)] * with_rim
            + [jax.ShapeDtypeStruct(size, jnp.bfloat16) for size in pieces],
            compiler_params=pltpu.CompilerParams(vmem_limit_bytes=VMEM),
            cost_estimate=pl.CostEstimate(
                flops=12_000_000_000, bytes_accessed=20_000_000, transcendentals=0
            ),
            name="form",
        )(hot, perm, pointing_table, signal, *([rim] if with_rim else []))

    edge, opening = form(groups[:1], signal, rim)
    pieces = [opening]
    if len(groups) > 1:
        later, _ = lax.optimization_barrier((signal, opening))
        pieces += form(groups[1:], later, None)

    mat = synthesis_matrix(filter_taps, inner, reach)

    edge = edge[:, :, :rim_len]
    edge = jnp.concatenate(
        [
            edge[:, 2 * devices * start : 2 * devices * (start + group)].reshape(
                local_subbands, devices, 2 * group * rim_len
            )
            for start, group in zip(starts, groups)
        ],
        axis=2,
    )
    edge = edge.swapaxes(0, 1).reshape(devices, -1)
    edge_size = edge.shape[1]
    planes = -(-edge_size // (2 * groups[0] * LANES))
    edge = jnp.pad(edge, ((0, 0), (0, planes * 2 * groups[0] * LANES - edge_size)))
    edge = edge.reshape(devices, planes, 2 * groups[0], LANES)
    pieces = [
        piece.reshape(devices, local_subbands * inner, 2 * group, LANES)
        for piece, group in zip(pieces, groups)
    ]
    pieces[0] = jnp.concatenate([pieces[0], edge], axis=1)
    got = [lax.all_to_all(p, "sub", split_axis=0, concat_axis=0, tiled=True) for p in pieces]
    edge = got[0][:, local_subbands * inner :].reshape(devices, -1)[:, :edge_size]
    edge = jnp.take(edge.reshape(slots, -1), subband_order, axis=0)
    live_mask = jnp.arange(slots, dtype=jnp.int32) < live_subbands[0]
    edge = jnp.where(live_mask[:, None], edge.astype(jnp.float32), 0.0)

    def edge_of(start, group):
        part = edge[:, 2 * start * rim_len : 2 * (start + group) * rim_len]
        part = part.reshape(bands, chan, 2, group, reach - 1, inner)
        return part.transpose(0, 3, 2, 4, 5, 1).reshape(
            bands, group, 2, reach - 1, inner * chan
        )

    result = None
    for first, start, group, z in zip(firsts, starts, groups, got):
        operands = [subband_order, live_subbands, z, edge_of(start, group), mat]
        in_specs = [
            pl.BlockSpec(memory_space=pl.ANY),
            pl.BlockSpec((1, group, 2, reach - 1, LANES), lambda g, *_: (g, 0, 0, 0, 0)),
            pl.BlockSpec(mat.shape, lambda g, *_: (0, 0)),
        ]
        alias = {}
        if result is not None:
            operands.append(result)
            in_specs.append(pl.BlockSpec(memory_space=pl.ANY))
            alias = {5: 0}
        result = pl.pallas_call(
            functools.partial(synth_kernel, inner, chan, group, reach, local_subbands),
            grid_spec=pltpu.PrefetchScalarGridSpec(
                num_scalar_prefetch=2,
                grid=(bands,),
                in_specs=in_specs,
                out_specs=pl.BlockSpec(
                    (group, 1, 2, local_time * chan), functools.partial(lambda h, g, *_: (h, g, 0, 0), first // group)
                ),
                scratch_shapes=[
                    pltpu.VMEM((2, chan, inner, 2 * group, LANES), jnp.bfloat16),
                    pltpu.VMEM((inner, chan * 2 * group, LANES), jnp.float32),
                    pltpu.VMEM((2, 8 + LANES, LANES), jnp.float32),
                    pltpu.VMEM((group * LANES, mat.shape[0]), jnp.bfloat16),
                    pltpu.VMEM((2, 2 * LANES, LANES), jnp.float32),
                    pltpu.SemaphoreType.DMA((2,)),
                ],
            ),
            out_shape=jax.ShapeDtypeStruct((beam_part, bands, 2, local_time * chan), jnp.bfloat16),
            input_output_aliases=alias,
            compiler_params=pltpu.CompilerParams(vmem_limit_bytes=VMEM),
            cost_estimate=pl.CostEstimate(
                flops=10_000_000_000, bytes_accessed=13_000_000, transcendentals=0
            ),
            name="synth",
        )(*operands)

    return result


def solution(mesh):
    in_specs = (P("sub", None, None, "tm"), P("sub", None, None, None), P(), P(), P(), P())
    out_specs = P("sub", None, None, "tm")
    return jax.shard_map(
        on_device, mesh=mesh, in_specs=in_specs, out_specs=out_specs, check_vma=False
    )
```
